32 devices in a mesh: row: 8 (over z, x), col: 4 (over y, core).
Axes of the slice: x: 2, y: 2, z: 4, core: 2. Of those that a mesh axis runs over, the one named last changes fastest.
Arguments:
- innovations: float32 [64, 16384], P(None, ('row', 'col')), may hold values from -300 to 300
- obs_factors: float32 [64, 16384], P(None, ('row', 'col')), may hold values from -6 to 6
- component: int32 [16384], P(('row', 'col')), may hold values 0 or 1
- obs_error: float32 [16384], P(('row', 'col')), may hold values from 0.5 to 2
- coupling: float32 [2, 2], replicated, may hold values from 0.5 to 2
- tile_slots: int32 [8, 4, 8, 3], P('row', 'col'), may hold values from 0 to 7, as said below
Outputs:
- increment: float32 [64, 16384], P(None, ('row', 'col'))
- residual: float32 [64, 16384], P(None, ('row', 'col'))
The draws below stay inside these ranges and needn't reach their ends.
Inputs may be any that keep to these rules, and one draw needn't show every extreme that they name: `tile_slots`: each device's slots name distinct (local block row, local block column) pairs; on some device all 8 slots are live; the live flag is 0 or 1; local block rows are below 4 and local block columns below 8.
All inputs are finite; a program needn't handle non-finite values. No bound on the sum of `component` on one device may be relied on, other than what follows from the above.
Results may differ from the reference program's by a relative error of at most 0.0003.
Values sent between devices are 32-bit elements; how exact they have to be, the bound alone decides.
A program may use at most 64 MiB of HBM per device.

```python
import math
import jax
import jax.numpy as jnp
from jax import lax

TILE = 512
DF = 64
NRHS = 64
ITERS = 3
SLOTS = 8
BLK_DEV = 1
ROW_DEVS = 8
COL_DEVS = 4
NR_LOC = 4
NC_LOC = 8
NOBS = 16384


def factor_field(key):
    factor_key = jax.random.fold_in(key, 7)
    field = jnp.clip(jax.random.normal(factor_key, (DF, NOBS), jnp.float32), -6.0, 6.0)
    return field


def draw_obs_factors(key, part):
    return factor_field(key)


def draw_innovations(key, part):
    first_key = jax.random.fold_in(jax.random.fold_in(key, 3), 0)
    third_key = jax.random.fold_in(jax.random.fold_in(key, 3), 2)
    position = jnp.arange(NOBS, dtype=jnp.float32) / NOBS
    rising = jnp.exp(math.log(3.0) * position)
    loadings = jax.random.normal(third_key, (NRHS, DF), jnp.float32)
    coherent = jnp.dot(loadings, factor_field(key), precision=lax.Precision.HIGHEST) / math.sqrt(DF)
    noise_part = jnp.clip(jax.random.normal(first_key, (NRHS, NOBS), jnp.float32), -6.0, 6.0)
    coherent = jnp.clip(coherent, -6.0, 6.0)
    mixed = 0.5 * noise_part + 0.85 * coherent
    return mixed * rising[None, :]


def draw_tile_slots(key, part):
    first_key, second_key, third_key = jax.random.split(jax.random.fold_in(key, 11), 3)
    devices = ROW_DEVS * COL_DEVS
    cells = NR_LOC * NC_LOC
    scores = jax.random.randint(first_key, (devices, cells), 0, 65536) * cells + jnp.arange(cells, dtype=jnp.int32)[None, :]
    chosen = jnp.argsort(scores, axis=1)[:, :SLOTS].astype(jnp.int32)
    spread = SLOTS - SLOTS // 6
    extra = jax.random.randint(second_key, (devices,), 0, spread + 1)
    counts = SLOTS // 6 + extra * extra // max(spread, 1)
    picked = jax.random.randint(third_key, (), 0, devices)
    counts = jnp.where(jnp.arange(devices, dtype=jnp.int32) == picked, SLOTS, counts)
    live_flags = (jnp.arange(SLOTS, dtype=jnp.int32)[None, :] < counts[:, None]).astype(jnp.int32)
    stacked = jnp.stack([chosen // NC_LOC, chosen % NC_LOC, live_flags], axis=-1)
    return stacked.reshape(ROW_DEVS, COL_DEVS, SLOTS, 3).astype(jnp.int32)


def with_ends(values, own_key, least, high):
    spot = [jax.random.randint(jax.random.fold_in(own_key, axis), (), 0, length) for axis, length in enumerate(values.shape)]
    widest = values.shape.index(max(values.shape))
    beside = spot[:widest] + [(spot[widest] + 1) % values.shape[widest]] + spot[widest + 1:]
    return values.at[tuple(spot)].set(least).at[tuple(beside)].set(high)


def levels(rng, dims, shards, smallest, largest):
    factor_of = 1.0
    for dim, shards_of in shards:
        heights = jax.random.uniform(jax.random.fold_in(jax.random.fold_in(rng, 6), dim), (shards_of,), jnp.float32, smallest / len(shards), largest / len(shards))
        factor_of = factor_of * jnp.repeat(jnp.exp(heights), dims[dim] // shards_of).reshape((-1,) + (1,) * (len(dims) - 1 - dim))
    return factor_of


def setup_inputs(seed: int = 0) -> dict:
    arg_keys = jax.random.split(jax.random.key(seed), 7)
    return {
        "innovations": draw_innovations(jax.random.fold_in(arg_keys[6], 71), 0),
        "obs_factors": draw_obs_factors(jax.random.fold_in(arg_keys[6], 71), 0),
        "component": with_ends((jax.random.randint(arg_keys[2], (NOBS,), 0, 4) < 1).astype(jnp.int32), jax.random.fold_in(arg_keys[2], 1), 0, 1),
        "obs_error": jnp.clip(jnp.exp(math.log(2.0) - 1.3862944 * jax.random.uniform(arg_keys[3], (NOBS,), jnp.float32) ** levels(arg_keys[3], (NOBS,), ((0, 32),), -0.2, 0.2)), 0.5, 2.0),
        "coupling": jnp.clip(jnp.exp(jax.random.uniform(arg_keys[4], (2, 2), jnp.float32, math.log(0.5), math.log(2.0))), 0.5, 2.0),
        "tile_slots": draw_tile_slots(jax.random.fold_in(arg_keys[6], 71), 0),
    }


length_sq = 12.0


def tile_matrix(left_factors, right_factors, left_labels, right_labels, coupling):
    left_norms = jnp.sum(left_factors * left_factors, axis=0)
    right_norms = jnp.sum(right_factors * right_factors, axis=0)
    products = lax.dot_general(left_factors, right_factors, (((0,), (0,)), ((), ())), precision=lax.Precision.HIGHEST, preferred_element_type=jnp.float32)
    pair_coupling = (1.0 - left_labels)[:, None] * ((1.0 - right_labels)[None, :] * coupling[0, 0] + right_labels[None, :] * coupling[0, 1]) + left_labels[:, None] * ((1.0 - right_labels)[None, :] * coupling[1, 0] + right_labels[None, :] * coupling[1, 1])
    return pair_coupling * jnp.exp(-(left_norms[:, None] + right_norms[None, :] - 2.0 * products) / length_sq)


def take_segment(array, block):
    start = (block * TILE).astype(jnp.int32)
    return lax.dynamic_slice_in_dim(array, start, TILE, array.ndim - 1)


def add_segment(vector, block, values):
    start = (block * TILE).astype(jnp.int32)
    last_axis = vector.ndim - 1
    before = lax.dynamic_slice_in_dim(vector, start, TILE, last_axis)
    return lax.dynamic_update_slice_in_dim(vector, before + values, start, last_axis)


def reference(innovations, obs_factors, component, obs_error, coupling, tile_slots):
    labels_float = component.astype(jnp.float32)
    row_devices = jnp.arange(ROW_DEVS, dtype=jnp.int32)[:, None, None]
    column_devices = jnp.arange(COL_DEVS, dtype=jnp.int32)[None, :, None]
    row_block = tile_slots[..., 0]
    column_block = tile_slots[..., 1]
    global_rows = ((row_devices * COL_DEVS + row_block // BLK_DEV) * BLK_DEV + row_block % BLK_DEV).reshape(-1).astype(jnp.int32)
    global_columns = (((column_block // BLK_DEV) * COL_DEVS + column_devices) * BLK_DEV + column_block % BLK_DEV).reshape(-1).astype(jnp.int32)
    live_list = tile_slots[..., 2].reshape(-1).astype(jnp.int32)

    def listed_tile(row_index, column_index):
        return tile_matrix(take_segment(obs_factors, row_index), take_segment(obs_factors, column_index), take_segment(labels_float, row_index), take_segment(labels_float, column_index), coupling)

    def weigh(totals, item):
        row_index, column_index, flag = item

        def work(totals):
            block_matrix = listed_tile(row_index, column_index)
            totals = add_segment(totals, row_index, jnp.sum(block_matrix, axis=1))
            return add_segment(totals, column_index, jnp.sum(block_matrix, axis=0))

        return lax.cond(flag > 0, work, lambda totals: totals, totals), None

    row_weights, unused = lax.scan(weigh, jnp.zeros((NOBS,), jnp.float32), (global_rows, global_columns, live_list))
    diagonal = obs_error + row_weights

    def operate(vector):
        def visit(totals, item):
            row_index, column_index, flag = item

            def work(totals):
                block_matrix = listed_tile(row_index, column_index)
                left_values = take_segment(vector, row_index)
                right_values = take_segment(vector, column_index)
                totals = add_segment(totals, row_index, lax.dot_general(right_values, block_matrix, (((1,), (1,)), ((), ())), precision=lax.Precision.HIGHEST, preferred_element_type=jnp.float32))
                return add_segment(totals, column_index, jnp.dot(left_values, block_matrix, precision=lax.Precision.HIGHEST, preferred_element_type=jnp.float32))

            return lax.cond(flag > 0, work, lambda totals: totals, totals), None

        image, unused = lax.scan(visit, jnp.zeros((NRHS, NOBS), jnp.float32), (global_rows, global_columns, live_list))
        return diagonal[None, :] * vector + image

    increment = jnp.zeros_like(innovations)
    residual = innovations
    direction = innovations
    norm_now = jnp.sum(residual * residual, axis=1)
    for repeat in range(ITERS):
        image = operate(direction)
        alpha = norm_now / jnp.sum(direction * image, axis=1)
        increment = increment + alpha[:, None] * direction
        residual = residual - alpha[:, None] * image
        norm_next = jnp.sum(residual * residual, axis=1)
        direction = residual + (norm_next / norm_now)[:, None] * direction
        norm_now = norm_next
    return increment, residual
```

```python
import functools
import math

import jax
import jax.numpy as jnp
from jax import lax
from jax.experimental import pallas as pl
from jax.experimental.pallas import tpu as pltpu
from jax.sharding import PartitionSpec as P

ITERS = 3
length_sq = 12.0
MESH = pl.DeviceIdType.MESH
VMEM = pl.BlockSpec(memory_space=pltpu.VMEM)
SMEM = pl.BlockSpec(memory_space=pltpu.SMEM)
F32, BF16 = jnp.float32, jnp.bfloat16
PIECE_FACTORS = 24
PIECE_FIRST = 24
PIECE = 16
EXTRA = 8
ONES = 16
DEAD = 1000.0


def legs(rows):
    outer = 4 if rows % 4 == 0 else rows
    return outer, rows // outer


def pieces(height, size):
    return [(start, min(size, height - start)) for start in range(0, height, size)]


def remote(src, dst, send, recv, device):
    return pltpu.make_async_remote_copy(
        src_ref=src, dst_ref=dst, send_sem=send, recv_sem=recv,
        device_id=device, device_id_type=MESH,
    )


def split2(x):
    top = x.astype(BF16)
    return top, (x - top.astype(F32)).astype(BF16)


def split3(x):
    first = x.astype(BF16)
    rest = x - first.astype(F32)
    second = rest.astype(BF16)
    return first, second, (rest - second.astype(F32)).astype(BF16)


def fold(x):
    total = x[:, :128]
    for start in range(128, x.shape[1], 128):
        total = total + x[:, start:start + 128]
    return total


def lane_sums(x):
    rest = 128 - x.shape[0]
    square = jnp.concatenate([x, jnp.zeros((rest, 128), F32)], axis=0) if rest else x
    return jnp.sum(jnp.transpose(square), axis=0, keepdims=True)


def column(row, height, width):
    square = jnp.transpose(jnp.broadcast_to(row, (128, 128)))[:height]
    return jnp.concatenate([square] * (width // 128), axis=1)


def stack_rows(values, width):
    place = lax.broadcasted_iota(jnp.int32, (16, width), 0)
    total = jnp.zeros((16, width), F32)
    for n, value in enumerate(values):
        total = jnp.where(place == n, value.astype(F32), total)
    return total.astype(BF16)


class Sends:
    def __init__(self):
        self.held = []

    def go(self, copy, when=None):
        if when is None:
            copy.start()
        else:
            pl.when(when)(copy.start)
        self.held.append((copy, when))

    def drain(self):
        for copy, when in self.held:
            if when is None:
                copy.wait_send()
            else:
                pl.when(when)(copy.wait_send)
        self.held = []


def kernel(rows, cols, innov, factors, labels, errors, coupling, slots, inc_out, res_out,
           f_row, f_col, v_row, v_col, d_row, d_col, x_row, x_col, left, t_high, t_low,
           col_part, row_part, where_slot, s1, s2,
           x_stage, x_got, z_stage, z_got, c_stage, c_got, product, diag, direction,
           gf_row, gf_col, gv_row, gv_col, hf_z, hf_x, hf_c, hv_z, hv_x, hv_c,
           rx, rz, rc, qx, qz, qc, r1, r2, q1, q2):
    r, c = lax.axis_index("row"), lax.axis_index("col")
    outer, inner = legs(rows)
    z, w = lax.div(r, inner), lax.rem(r, inner)
    has_low, has_high = z > 0, z < outer - 1
    low, high = (r - inner, c), (r + inner, c)
    to_col = [(r, lax.rem(c + k, cols)) for k in range(1, cols)]
    to_row = [(lax.rem(r + k, rows), c) for k in range(1, rows)]
    from_col = [lax.rem(c + cols - k, cols) for k in range(1, cols)]
    from_row = [lax.rem(r + rows - k, rows) for k in range(1, rows)]
    side_of = [lax.rem(w + j, inner) for j in range(1, inner)]
    back_of = [lax.rem(w + inner - j, inner) for j in range(1, inner)]
    rhs, tile = innov.shape
    depth = factors.shape[0]
    count = slots.shape[0]

    def gather_start(sends, source, row_buf, col_buf, parts, g_row, g_col, h_z, h_x, h_c):
        for n, (start, size) in enumerate(parts):
            span = pl.ds(start, size)
            mine = source.at[span]
            target = row_buf.at[r, span]
            sends.go(remote(mine, target, h_z.at[0, 0, n], g_row.at[r, n], low), has_low)
            sends.go(remote(mine, target, h_z.at[1, 0, n], g_row.at[r, n], high), has_high)
            for j, side in enumerate(side_of):
                sends.go(remote(mine, target, h_x.at[0, 0, j, n], g_row.at[r, n],
                                (z * inner + side, c)))
            for k, device in enumerate(to_col):
                sends.go(remote(mine, col_buf.at[c, span], h_c.at[k, n], g_col.at[c, n], device))

    def gather_relay(sends, row_buf, parts, g_row, h_z, h_x):
        for step in range(1, outer):
            for n, (start, size) in enumerate(parts):
                span = pl.ds(start, size)
                for way in range(2):
                    slot = r - step * inner if way else r + step * inner
                    there = z - step >= 0 if way else z + step < outer
                    onward = has_high if way else has_low
                    block = row_buf.at[slot, span]
                    arrival = remote(block, block, h_z.at[way, step, n], g_row.at[slot, n],
                                     high if way else low)
                    pl.when(there)(arrival.wait_recv)
                    sends.go(arrival, there & onward)
                    for j, side in enumerate(side_of):
                        sends.go(remote(block, block, h_x.at[way, step, j, n], g_row.at[slot, n],
                                        (z * inner + side, c)), there)
            yield step

    def gather_finish(row_buf, col_buf, parts, g_row, g_col, h_x, h_c):
        for n, (start, size) in enumerate(parts):
            span = pl.ds(start, size)
            for k, q in enumerate(from_col):
                block = col_buf.at[q, span]
                remote(block, block, h_c.at[k, n], g_col.at[q, n], to_col[k]).wait_recv()
        for n, (start, size) in enumerate(parts):
            span = pl.ds(start, size)
            for plane in range(outer):
                for j, back in enumerate(back_of):
                    slot = plane * inner + back
                    block = row_buf.at[slot, span]
                    remote(block, block, h_x.at[0, 0, j, n], g_row.at[slot, n],
                           (z * inner + back, c)).wait_recv()

    def small_start(sends, kind, value):
        s1[kind, c] = jnp.broadcast_to(value, (8, 128))
        for k, device in enumerate(to_col):
            sends.go(remote(s1.at[kind, c], s1.at[kind, c], q1.at[kind, k], r1.at[kind, k], device))

    def small_middle(sends, kind):
        for k, q in enumerate(from_col):
            remote(s1.at[kind, q], s1.at[kind, q], q1.at[kind, k], r1.at[kind, k],
                   to_col[k]).wait_recv()
        s2[kind, r] = jnp.sum(s1[kind], axis=0)
        for k, device in enumerate(to_row):
            sends.go(remote(s2.at[kind, r], s2.at[kind, r], q2.at[kind, k], r2.at[kind, k], device))

    def small_end(kind):
        for k, q in enumerate(from_row):
            remote(s2.at[kind, q], s2.at[kind, q], q2.at[kind, k], r2.at[kind, k],
                   to_row[k]).wait_recv()
        return jnp.sum(s2[kind], axis=0)[:1]

    barrier = pltpu.get_barrier_semaphore()
    for device in to_col + to_row:
        pl.semaphore_signal(barrier, inc=1, device_id=device, device_id_type=MESH)

    scale = math.sqrt(2.0 / (length_sq * math.log(2.0)))
    own = jnp.concatenate(
        [factors[...] * scale, jnp.broadcast_to(labels[...].astype(F32), (EXTRA, tile))], axis=0
    )
    f_row[r] = own
    f_col[c] = own
    start_values = innov[...]
    rr_part = lane_sums(fold(start_values * start_values))
    pl.semaphore_wait(barrier, len(to_col) + len(to_row))

    f_parts = pieces(depth + EXTRA, PIECE_FACTORS)
    v_parts = pieces(rhs, PIECE)
    sends_f, sends_v, sends_s, sends_r = Sends(), Sends(), Sends(), Sends()
    gather_start(sends_f, f_row.at[r], f_row, f_col, f_parts, gf_row, gf_col, hf_z, hf_x, hf_c)
    small_start(sends_s, 0, rr_part)
    gather_start(sends_v, innov, v_row.at[0], v_col.at[0], v_parts,
                 gv_row, gv_col, hv_z, hv_x, hv_c)

    v_row[0, r] = start_values
    v_col[0, c] = start_values
    direction[...] = start_values
    inc_out[...] = jnp.zeros_like(start_values)
    res_out[...] = start_values
    for part in (col_part, row_part):
        part[count] = jnp.zeros(part.shape[1:], F32)

    def locate(n, carry):
        a, b = lax.div(n, rows), lax.rem(n, rows)
        found = jnp.int32(count)
        for s in range(count):
            hit = (slots[s, 2] > 0) & (slots[s, 0] == a) & (slots[s, 1] == b)
            found = jnp.where(hit, s, found)
        where_slot[n] = found
        return carry

    lax.fori_loop(0, rows * cols, locate, 0)

    logs = [[jnp.log(jnp.full((1, tile), coupling[i, j], F32)) * (1.0 / math.log(2.0))
             for j in range(2)] for i in range(2)]
    one = jnp.ones((1, tile), F32)
    nothing = jnp.zeros((tile - 6 * depth - 16, tile), BF16)

    relay_f = gather_relay(sends_f, f_row, f_parts, gf_row, hf_z, hf_x)
    next(relay_f)
    small_middle(sends_s, 0)
    for n, (start, size) in enumerate(f_parts):
        for k, q in enumerate(from_col):
            block = f_col.at[q, pl.ds(start, size)]
            remote(block, block, hf_c.at[k, n], gf_col.at[q, n], to_col[k]).wait_recv()

    def prepare(a, carry):
        g = f_col[a, :depth]
        label = f_col[a, depth:depth + 1]
        g1, g2, g3 = split3(g)
        m = split3(-0.5 * jnp.sum(g * g, axis=0, keepdims=True))
        extra = stack_rows(list(m) + [one] * 3 + [label] * 3, tile)
        stack = jnp.concatenate([g1, g1, g2, g2, g1, g3, extra, nothing], axis=0)
        left[a] = jnp.transpose(stack)
        return carry

    lax.fori_loop(0, cols, prepare, 0)
    for _ in relay_f:
        pass
    for n, (start, size) in enumerate(f_parts):
        span = pl.ds(start, size)
        for plane in range(outer):
            for j, back in enumerate(back_of):
                slot = plane * inner + back
                block = f_row.at[slot, span]
                remote(block, block, hf_x.at[0, 0, j, n], gf_row.at[slot, n],
                       (z * inner + back, c)).wait_recv()

    def build(s, carry):
        a, b = slots[s, 0], slots[s, 1]
        g = f_row[b, :depth]
        label = f_row[b, depth:depth + 1]
        g1, g2, g3 = split3(g)
        gone = jnp.where(slots[s, 2] > 0, 0.0, DEAD)
        base = -0.5 * jnp.sum(g * g, axis=0, keepdims=True)
        base = base + (logs[0][0] + label * (logs[0][1] - logs[0][0])) - gone
        slope = (logs[1][0] - logs[0][0]) + label * (
            (logs[1][1] - logs[1][0]) - (logs[0][1] - logs[0][0]))
        extra = stack_rows([one] * 3 + list(split3(base)) + list(split3(slope)), tile)
        stack = jnp.concatenate([g1, g2, g1, g2, g3, g1, extra, nothing], axis=0)
        value = jnp.exp2(jnp.dot(left[a], stack, preferred_element_type=F32))
        top, rest = split2(value)
        t_high[s] = top
        t_low[s] = rest
        return carry

    relay_v = gather_relay(sends_v, v_row.at[0], v_parts, gv_row, hv_z, hv_x)
    half = count // 2
    lax.fori_loop(0, half, build, 0)
    next(relay_v)
    lax.fori_loop(half, count, build, 0)
    for _ in relay_v:
        pass
    gather_finish(v_row.at[0], v_col.at[0], v_parts, gv_row, gv_col, hv_x, hv_c)
    norm_now = small_end(0)
    sends_f.drain()

    ones_rows = jnp.ones((ONES, tile), BF16)
    bottom = rhs + ONES

    def put(target, index, value):
        top, rest = split2(value)
        target[index, :rhs] = top
        target[index, rhs:bottom] = ones_rows
        target[index, bottom:] = rest

    def sweep(s, carry):
        a, b = slots[s, 0], slots[s, 1]
        for values, index, side, part in ((x_row, b, 1, row_part), (x_col, a, 0, col_part)):
            dims = (((1,), (side,)), ((), ()))
            wide = lax.dot_general(values[index], t_high[s], dims, preferred_element_type=F32)
            rest = lax.dot_general(values[index, :bottom], t_low[s], dims,
                                   preferred_element_type=F32)
            part[s, :rhs] = wide[:rhs] + (wide[bottom:] + rest[:rhs])
            part[s, rhs:] = wide[rhs:rhs + EXTRA] + rest[rhs:rhs + EXTRA]
        return carry

    def column_image(b, span):
        total = col_part[where_slot[b], span]
        for a in range(1, cols):
            total = total + col_part[where_slot[a * rows + b], span]
        return total

    def row_image(a, span):
        total = row_part[where_slot[a * rows], span]
        for b in range(1, rows):
            total = total + row_part[where_slot[a * rows + b], span]
        return total

    order = []
    lower_half = z < outer // 2
    for i in range(outer - 1):
        down = outer - 1 - i
        order.append(jnp.where(lower_half, jnp.where(down <= z, down - 1, down),
                               jnp.where(i >= z, i + 1, i)))
    order.append(z)

    for repeat in range(ITERS):
        first = repeat == 0
        if first:
            def ready_row(b, carry):
                put(x_row, b, v_row[0, b])
                return carry

            def ready_col(a, carry):
                put(x_col, a, v_col[0, a])
                return carry
        else:
            old_row = v_row.at[0] if repeat == 1 else d_row
            old_col = v_col.at[0] if repeat == 1 else d_col
            weight = column(beta, rhs, tile)

            def ready_row(b, carry):
                value = v_row[repeat, b] + weight * old_row[b]
                d_row[b] = value
                put(x_row, b, value)
                return carry

            def ready_col(a, carry):
                value = v_col[repeat, a] + weight * old_col[a]
                d_col[a] = value
                put(x_col, a, value)
                return carry

        lax.fori_loop(0, rows, ready_row, 0)
        lax.fori_loop(0, cols, ready_col, 0)
        lax.fori_loop(0, count, sweep, 0)

        held_col = v_col.at[0] if first else d_col
        held_row = v_row.at[0] if first else d_row
        parts = pieces(rhs + EXTRA, PIECE_FIRST) if first else pieces(rhs, PIECE)
        sends_r.drain()
        sends_s.drain()

        def send_across(i):
            for j, side in enumerate(side_of):
                for n, (start, size) in enumerate(parts):
                    span = pl.ds(start, size)
                    x_stage[i, j, span] = column_image(order[i] * inner + side, span)
                    sends_r.go(remote(x_stage.at[i, j, span], x_got.at[i, j, span],
                                      qx.at[i, j, n], rx.at[i, j, n], (z * inner + side, c)))

        def joined(i, n, span):
            value = column_image(order[i] * inner + w, span)
            for j in range(inner - 1):
                block = x_got.at[i, j, span]
                remote(block, block, qx.at[i, j, n], rx.at[i, j, n],
                       (z * inner + side_of[j], c)).wait_recv()
                value = value + x_got[i, j, span]
            return value

        send_across(0)
        own_err = errors[...] if first else diag[...]
        here = direction[...]
        dots = fold(own_err * here * here)
        for k in range(cols):
            a = to_col[k][1] if k < cols - 1 else c
            for n, (start, size) in enumerate(parts):
                span = pl.ds(start, size)
                value = row_image(a, span)
                c_stage[k, span] = value
                if k < cols - 1:
                    sends_r.go(remote(c_stage.at[k, span], c_got.at[k, span],
                                      qc.at[k, n], rc.at[k, n], to_col[k]))
            held = held_col[a]
            dots = dots + 2.0 * fold(c_stage[k, :rhs] * held)
            if first:
                dots = dots + fold(c_stage[k, rhs:rhs + 1] * (held * held))
        if first:
            def weigh(b, carry):
                held = held_row[b]
                return carry + fold(column_image(b, pl.ds(rhs, EXTRA))[:1] * (held * held))

            dots = lax.fori_loop(0, rows, weigh, dots)
        small_start(sends_s, 1, lane_sums(dots))
        for i in range(1, outer):
            send_across(i)
        small_middle(sends_s, 1)

        for i in range(outer - 1):
            q = order[i]
            below = q < z
            way = jnp.where(below, 0, 1)
            more = jnp.where(below, z + 1 < outer, z > 0)
            target = (jnp.where(below, r - inner, r + inner), c)
            for n, (start, size) in enumerate(parts):
                span = pl.ds(start, size)
                z_stage[i, span] = joined(i, n, span)
                copy = remote(z_stage.at[i, span], z_got.at[way, q, span],
                              qz.at[i, n], rz.at[way, q, n], target)

                @pl.when(more)
                def _():
                    copy.wait_recv()
                    z_stage[i, span] += z_got[way, q, span]

                sends_r.go(copy)
        for n, (start, size) in enumerate(parts):
            span = pl.ds(start, size)
            for k, q in enumerate(from_col):
                block = c_got.at[k, span]
                remote(block, block, qc.at[k, n], rc.at[k, n], to_col[k]).wait_recv()
            value = c_stage[cols - 1, span]
            for k in range(cols - 1):
                value = value + c_got[k, span]
            product[span] = value + joined(outer - 1, n, span)
            for way, there in enumerate((has_high, has_low)):
                @pl.when(there)
                def _():
                    block = z_got.at[way, z, span]
                    remote(block, block, qz.at[0, n], rz.at[way, z, n],
                           high if way == 0 else low).wait_recv()
                    product[span] += z_got[way, z, span]
        alpha = norm_now / small_end(1)
        step = column(alpha, rhs, tile)
        if first:
            diag[...] = errors[...] + product[rhs:rhs + 1]
        image = diag[...] * here + product[:rhs]
        inc_out[...] += step * here
        residual = res_out[...] - step * image
        res_out[...] = residual
        sends_v.drain()
        if repeat + 1 < ITERS:
            v_row[repeat + 1, r] = residual
            v_col[repeat + 1, c] = residual
            row_buf, col_buf = v_row.at[repeat + 1], v_col.at[repeat + 1]
            gather_start(sends_v, row_buf.at[r], row_buf, col_buf, v_parts,
                         gv_row, gv_col, hv_z, hv_x, hv_c)
            sends_s.drain()
            small_start(sends_s, 0, lane_sums(fold(residual * residual)))
            relay = gather_relay(sends_v, row_buf, v_parts, gv_row, hv_z, hv_x)
            next(relay)
            small_middle(sends_s, 0)
            for _ in relay:
                pass
            gather_finish(row_buf, col_buf, v_parts, gv_row, gv_col, hv_x, hv_c)
            norm_next = small_end(0)
            beta = norm_next / norm_now
            norm_now = norm_next
            direction[...] = residual + column(beta, rhs, tile) * here
    sends_r.drain()
    sends_s.drain()
    sends_v.drain()


def shards(rows, cols, innovations, obs_factors, component, obs_error, coupling, tile_slots):
    slots = tile_slots[0, 0]
    rhs, tile = innovations.shape
    depth = obs_factors.shape[0]
    count = slots.shape[0]
    outer, inner = legs(rows)
    sides = max(inner - 1, 1)
    tall, wide = depth + EXTRA, rhs + EXTRA
    nf = len(pieces(tall, PIECE_FACTORS))
    nv = len(pieces(rhs, PIECE))
    nr = max(len(pieces(wide, PIECE_FIRST)), nv)
    dma = pltpu.SemaphoreType.DMA
    scratch = [
        pltpu.VMEM((rows, tall, tile), F32),
        pltpu.VMEM((cols, tall, tile), F32),
        pltpu.VMEM((ITERS, rows, rhs, tile), F32),
        pltpu.VMEM((ITERS, cols, rhs, tile), F32),
        pltpu.VMEM((rows, rhs, tile), F32),
        pltpu.VMEM((cols, rhs, tile), F32),
        pltpu.VMEM((rows, 2 * rhs + ONES, tile), BF16),
        pltpu.VMEM((cols, 2 * rhs + ONES, tile), BF16),
        pltpu.VMEM((cols, tile, tile), BF16),
        pltpu.VMEM((count, tile, tile), BF16),
        pltpu.VMEM((count, tile, tile), BF16),
        pltpu.VMEM((count + 1, wide, tile), F32),
        pltpu.VMEM((count + 1, wide, tile), F32),
        pltpu.SMEM((rows * cols,), jnp.int32),
        pltpu.VMEM((2, cols, 8, 128), F32),
        pltpu.VMEM((2, rows, 8, 128), F32),
        pltpu.VMEM((outer, sides, wide, tile), F32),
        pltpu.VMEM((outer, sides, wide, tile), F32),
        pltpu.VMEM((outer, wide, tile), F32),
        pltpu.VMEM((2, outer, wide, tile), F32),
        pltpu.VMEM((cols, wide, tile), F32),
        pltpu.VMEM((cols, wide, tile), F32),
        pltpu.VMEM((wide, tile), F32),
        pltpu.VMEM((1, tile), F32),
        pltpu.VMEM((rhs, tile), F32),
        dma((rows, nf)), dma((cols, nf)), dma((rows, nv)), dma((cols, nv)),
        dma((2, outer, nf)), dma((2, outer, sides, nf)), dma((cols, nf)),
        dma((2, outer, nv)), dma((2, outer, sides, nv)), dma((cols, nv)),
        dma((outer, sides, nr)), dma((2, outer, nr)), dma((cols, nr)),
        dma((outer, sides, nr)), dma((outer, nr)), dma((cols, nr)),
        dma((2, cols)), dma((2, rows)), dma((2, cols)), dma((2, rows)),
    ]
    out = jax.ShapeDtypeStruct((rhs, tile), F32)
    return pl.pallas_call(
        functools.partial(kernel, rows, cols),
        out_shape=(out, out),
        in_specs=[VMEM] * 4 + [SMEM] * 2,
        out_specs=(VMEM, VMEM),
        scratch_shapes=scratch,
        compiler_params=pltpu.CompilerParams(collective_id=0, has_side_effects=True),
    )(innovations, obs_factors, component.reshape(1, tile), obs_error.reshape(1, tile),
      coupling, slots)


def solution(mesh):
    return jax.shard_map(
        functools.partial(shards, mesh.shape["row"], mesh.shape["col"]),
        mesh=mesh,
        in_specs=(
            P(None, ("row", "col")),
            P(None, ("row", "col")),
            P(("row", "col")),
            P(("row", "col")),
            P(),
            P("row", "col", None, None),
        ),
        out_specs=(P(None, ("row", "col")), P(None, ("row", "col"))),
        check_vma=False,
    )
```

```python
import functools
import math

import jax
import jax.numpy as jnp
from jax import lax
from jax.experimental import pallas as pl
from jax.experimental.pallas import tpu as pltpu
from jax.sharding import PartitionSpec as P

ITERS = 3
length_sq = 12.0
MESH = pl.DeviceIdType.MESH
VMEM = pl.BlockSpec(memory_space=pltpu.VMEM)
SMEM = pl.BlockSpec(memory_space=pltpu.SMEM)
F32, BF16 = jnp.float32, jnp.bfloat16
PIECE_FACTORS = 24
PIECE_FIRST = 24
PIECE = 16
EXTRA = 8
ONES = 16
DEAD = 1000.0


def legs(rows):
    outer = 4 if rows % 4 == 0 else rows
    return outer, rows // outer


def pieces(height, size):
    return [(start, min(size, height - start)) for start in range(0, height, size)]


def remote(src, dst, send, recv, device):
    return pltpu.make_async_remote_copy(
        src_ref=src, dst_ref=dst, send_sem=send, recv_sem=recv,
        device_id=device, device_id_type=MESH,
    )


def split2(x):
    top = x.astype(BF16)
    return top, (x - top.astype(F32)).astype(BF16)


def split3(x):
    first = x.astype(BF16)
    rest = x - first.astype(F32)
    second = rest.astype(BF16)
    return first, second, (rest - second.astype(F32)).astype(BF16)


def fold(x):
    total = x[:, :128]
    for start in range(128, x.shape[1], 128):
        total = total + x[:, start:start + 128]
    return total


def lane_sums(x):
    rest = 128 - x.shape[0]
    square = jnp.concatenate([x, jnp.zeros((rest, 128), F32)], axis=0) if rest else x
    return jnp.sum(jnp.transpose(square), axis=0, keepdims=True)


def column(row, height, width):
    square = jnp.transpose(jnp.broadcast_to(row, (128, 128)))[:height]
    return jnp.concatenate([square] * (width // 128), axis=1)


def stack_rows(values, width):
    place = lax.broadcasted_iota(jnp.int32, (16, width), 0)
    total = jnp.zeros((16, width), F32)
    for n, value in enumerate(values):
        total = jnp.where(place == n, value.astype(F32), total)
    return total.astype(BF16)


class Sends:
    def __init__(self):
        self.held = []

    def go(self, copy, when=None):
        if when is None:
            copy.start()
        else:
            pl.when(when)(copy.start)
        self.held.append((copy, when))

    def drain(self):
        for copy, when in self.held:
            if when is None:
                copy.wait_send()
            else:
                pl.when(when)(copy.wait_send)
        self.held = []


def kernel(rows, cols, innov, factors, labels, errors, coupling, slots, inc_out, res_out,
           f_row, f_col, v_row, v_col, d_row, d_col, x_row, x_col, left, t_high, t_low,
           col_part, row_part, where_slot, s1, s2,
           x_stage, x_got, z_stage, z_got, c_stage, c_got, product, diag, direction,
           gf_row, gf_col, gv_row, gv_col, hf_z, hf_x, hf_c, hv_z, hv_x, hv_c,
           rx, rz, rc, qx, qz, qc, r1, r2, q1, q2):
    r, c = lax.axis_index("row"), lax.axis_index("col")
    outer, inner = legs(rows)
    z, w = lax.div(r, inner), lax.rem(r, inner)
    has_low, has_high = z > 0, z < outer - 1
    low, high = (r - inner, c), (r + inner, c)
    to_col = [(r, lax.rem(c + k, cols)) for k in range(1, cols)]
    to_row = [(lax.rem(r + k, rows), c) for k in range(1, rows)]
    from_col = [lax.rem(c + cols - k, cols) for k in range(1, cols)]
    from_row = [lax.rem(r + rows - k, rows) for k in range(1, rows)]
    side_of = [lax.rem(w + j, inner) for j in range(1, inner)]
    back_of = [lax.rem(w + inner - j, inner) for j in range(1, inner)]
    rhs, tile = innov.shape
    depth = factors.shape[0]
    count = slots.shape[0]

    def gather_start(sends, source, row_buf, col_buf, parts, g_row, g_col, h_z, h_x, h_c):
        for n, (start, size) in enumerate(parts):
            span = pl.ds(start, size)
            mine = source.at[span]
            target = row_buf.at[r, span]
            sends.go(remote(mine, target, h_z.at[0, 0, n], g_row.at[r, n], low), has_low)
            sends.go(remote(mine, target, h_z.at[1, 0, n], g_row.at[r, n], high), has_high)
            for j, side in enumerate(side_of):
                sends.go(remote(mine, target, h_x.at[0, 0, j, n], g_row.at[r, n],
                                (z * inner + side, c)))
            for k, device in enumerate(to_col):
                sends.go(remote(mine, col_buf.at[c, span], h_c.at[k, n], g_col.at[c, n], device))

    def gather_relay(sends, row_buf, parts, g_row, h_z, h_x):
        for step in range(1, outer):
            for n, (start, size) in enumerate(parts):
                span = pl.ds(start, size)
                for way in range(2):
                    slot = r - step * inner if way else r + step * inner
                    there = z - step >= 0 if way else z + step < outer
                    onward = has_high if way else has_low
                    block = row_buf.at[slot, span]
                    arrival = remote(block, block, h_z.at[way, step, n], g_row.at[slot, n],
                                     high if way else low)
                    pl.when(there)(arrival.wait_recv)
                    sends.go(arrival, there & onward)
                    for j, side in enumerate(side_of):
                        sends.go(remote(block, block, h_x.at[way, step, j, n], g_row.at[slot, n],
                                        (z * inner + side, c)), there)
            yield step

    def gather_cols(col_buf, parts, g_col, h_c):
        for n, (start, size) in enumerate(parts):
            for k, q in enumerate(from_col):
                block = col_buf.at[q, pl.ds(start, size)]
                remote(block, block, h_c.at[k, n], g_col.at[q, n], to_col[k]).wait_recv()

    def gather_rows(row_buf, parts, g_row, h_x):
        for n, (start, size) in enumerate(parts):
            for plane in range(outer):
                for j, back in enumerate(back_of):
                    slot = plane * inner + back
                    block = row_buf.at[slot, pl.ds(start, size)]
                    remote(block, block, h_x.at[0, 0, j, n], g_row.at[slot, n],
                           (z * inner + back, c)).wait_recv()

    def small_start(sends, kind, value):
        s1[kind, c] = jnp.broadcast_to(value, (8, 128))
        mine = s1.at[kind, c, pl.ds(0, 1)]
        for k, device in enumerate(to_col):
            sends.go(remote(mine, mine, q1.at[kind, k], r1.at[kind, k], device))

    def small_middle(sends, kind):
        for k, q in enumerate(from_col):
            there = s1.at[kind, q, pl.ds(0, 1)]
            remote(there, there, q1.at[kind, k], r1.at[kind, k], to_col[k]).wait_recv()
        total = s1[kind, 0, :1]
        for k in range(1, cols):
            total = total + s1[kind, k, :1]
        s2[kind, r] = jnp.broadcast_to(total, (8, 128))
        mine = s2.at[kind, r, pl.ds(0, 1)]
        for k, device in enumerate(to_row):
            sends.go(remote(mine, mine, q2.at[kind, k], r2.at[kind, k], device))

    def small_end(kind):
        for k, q in enumerate(from_row):
            there = s2.at[kind, q, pl.ds(0, 1)]
            remote(there, there, q2.at[kind, k], r2.at[kind, k], to_row[k]).wait_recv()
        total = s2[kind, 0, :1]
        for k in range(1, rows):
            total = total + s2[kind, k, :1]
        return total

    barrier = pltpu.get_barrier_semaphore()
    for device in to_col + to_row:
        pl.semaphore_signal(barrier, inc=1, device_id=device, device_id_type=MESH)

    scale = math.sqrt(2.0 / (length_sq * math.log(2.0)))
    own = jnp.concatenate(
        [factors[...] * scale, jnp.broadcast_to(labels[...].astype(F32), (EXTRA, tile))], axis=0
    )
    f_row[r] = own
    f_col[c] = own
    start_values = innov[...]
    rr_part = lane_sums(fold(start_values * start_values))
    pl.semaphore_wait(barrier, len(to_col) + len(to_row))

    f_parts = pieces(depth + EXTRA, PIECE_FACTORS)
    v_parts = pieces(rhs, PIECE)
    sends_f, sends_v, sends_s, sends_r = Sends(), Sends(), Sends(), Sends()
    small_start(sends_s, 0, rr_part)
    gather_start(sends_f, f_row.at[r], f_row, f_col, f_parts, gf_row, gf_col, hf_z, hf_x, hf_c)
    gather_start(sends_v, innov, v_row.at[0], v_col.at[0], v_parts,
                 gv_row, gv_col, hv_z, hv_x, hv_c)

    v_row[0, r] = start_values
    v_col[0, c] = start_values
    direction[...] = start_values
    inc_out[...] = jnp.zeros_like(start_values)
    res_out[...] = start_values
    for part in (col_part, row_part):
        part[count] = jnp.zeros(part.shape[1:], F32)

    def locate(n, carry):
        a, b = lax.div(n, rows), lax.rem(n, rows)
        found = jnp.int32(count)
        for s in range(count):
            hit = (slots[s, 2] > 0) & (slots[s, 0] == a) & (slots[s, 1] == b)
            found = jnp.where(hit, s, found)
        where_slot[n] = found
        return carry

    lax.fori_loop(0, rows * cols, locate, 0)

    logs = [[jnp.log(jnp.full((1, tile), coupling[i, j], F32)) * (1.0 / math.log(2.0))
             for j in range(2)] for i in range(2)]
    one = jnp.ones((1, tile), F32)
    nothing = jnp.zeros((tile - 6 * depth - 16, tile), BF16)

    relay_f = gather_relay(sends_f, f_row, f_parts, gf_row, hf_z, hf_x)
    next(relay_f)
    small_middle(sends_s, 0)
    gather_cols(f_col, f_parts, gf_col, hf_c)

    def prepare(a, carry):
        g = f_col[a, :depth]
        label = f_col[a, depth:depth + 1]
        g1, g2, g3 = split3(g)
        m = split3(-0.5 * jnp.sum(g * g, axis=0, keepdims=True))
        extra = stack_rows(list(m) + [one] * 3 + [label] * 3, tile)
        stack = jnp.concatenate([g1, g1, g2, g2, g1, g3, extra, nothing], axis=0)
        left[a] = jnp.transpose(stack)
        return carry

    lax.fori_loop(0, cols, prepare, 0)
    for _ in relay_f:
        pass
    relay = gather_relay(sends_v, v_row.at[0], v_parts, gv_row, hv_z, hv_x)
    next(relay)
    gather_rows(f_row, f_parts, gf_row, hf_x)

    def build(s, carry):
        a, b = slots[s, 0], slots[s, 1]
        g = f_row[b, :depth]
        label = f_row[b, depth:depth + 1]
        g1, g2, g3 = split3(g)
        gone = jnp.where(slots[s, 2] > 0, 0.0, DEAD)
        base = -0.5 * jnp.sum(g * g, axis=0, keepdims=True)
        base = base + (logs[0][0] + label * (logs[0][1] - logs[0][0])) - gone
        slope = (logs[1][0] - logs[0][0]) + label * (
            (logs[1][1] - logs[1][0]) - (logs[0][1] - logs[0][0]))
        extra = stack_rows([one] * 3 + list(split3(base)) + list(split3(slope)), tile)
        stack = jnp.concatenate([g1, g2, g1, g2, g3, g1, extra, nothing], axis=0)
        value = jnp.exp2(jnp.dot(left[a], stack, preferred_element_type=F32))
        top, rest = split2(value)
        t_high[s] = top
        t_low[s] = rest
        return carry

    half = count // 2
    lax.fori_loop(0, half, build, 0)
    next(relay)
    lax.fori_loop(half, count, build, 0)

    ones_rows = jnp.ones((ONES, tile), BF16)
    bottom = rhs + ONES

    def put(target, index, value):
        top, rest = split2(value)
        target[index, :rhs] = top
        target[index, rhs:bottom] = ones_rows
        target[index, bottom:] = rest

    def sweep(values, which, side, part, begin, end):
        dims = (((1,), (side,)), ((), ()))

        def one_slot(s, carry):
            index = slots[s, which]
            wide = lax.dot_general(values[index], t_high[s], dims, preferred_element_type=F32)
            rest = lax.dot_general(values[index, :bottom], t_low[s], dims,
                                   preferred_element_type=F32)
            part[s, :rhs] = wide[:rhs] + (wide[bottom:] + rest[:rhs])
            part[s, rhs:] = wide[rhs:rhs + EXTRA] + rest[rhs:rhs + EXTRA]
            return carry

        lax.fori_loop(begin, end, one_slot, 0)

    def column_image(b, span):
        total = col_part[where_slot[b], span]
        for a in range(1, cols):
            total = total + col_part[where_slot[a * rows + b], span]
        return total

    def row_image(a, span):
        total = row_part[where_slot[a * rows], span]
        for b in range(1, rows):
            total = total + row_part[where_slot[a * rows + b], span]
        return total

    order = []
    lower_half = z < outer // 2
    for i in range(outer - 1):
        down = outer - 1 - i
        order.append(jnp.where(lower_half, jnp.where(down <= z, down - 1, down),
                               jnp.where(i >= z, i + 1, i)))
    order.append(z)

    for repeat in range(ITERS):
        first = repeat == 0
        row_buf, col_buf = v_row.at[repeat], v_col.at[repeat]
        parts = pieces(rhs + EXTRA, PIECE_FIRST) if first else pieces(rhs, PIECE)
        if not first:
            next(relay)
            small_middle(sends_s, 0)
            next(relay)
        gather_cols(col_buf, v_parts, gv_col, hv_c)
        weight = None
        if not first:
            norm_next = small_end(0)
            weight = column(norm_next / norm_now, rhs, tile)
            norm_now = norm_next
            direction[...] = res_out[...] + weight * direction[...]

        def ready(fresh, kept, target):
            def one_block(b, carry):
                value = fresh[repeat, b]
                if repeat:
                    value = value + weight * (fresh[0, b] if repeat == 1 else kept[b])
                    kept[b] = value
                put(target, b, value)
                return carry

            return one_block

        lax.fori_loop(0, cols, ready(v_col, d_col, x_col), 0)
        sweep(x_col, 0, 0, col_part, 0, half)
        for _ in relay:
            pass
        sweep(x_col, 0, 0, col_part, half, count)
        held_col = v_col.at[0] if first else d_col
        held_row = v_row.at[0] if first else d_row
        sends_r.drain()

        def send_across(i):
            for j, side in enumerate(side_of):
                for n, (start, size) in enumerate(parts):
                    span = pl.ds(start, size)
                    x_stage[i, j, span] = column_image(order[i] * inner + side, span)
                    sends_r.go(remote(x_stage.at[i, j, span], x_got.at[repeat, i, j, span],
                                      qx.at[i, j, n], rx.at[repeat, i, j, n], (z * inner + side, c)))

        def joined(i, n, span):
            value = column_image(order[i] * inner + w, span)
            for j in range(inner - 1):
                block = x_got.at[repeat, i, j, span]
                remote(block, block, qx.at[i, j, n], rx.at[repeat, i, j, n],
                       (z * inner + side_of[j], c)).wait_recv()
                value = value + x_got[repeat, i, j, span]
            return value

        for i in range(outer):
            send_across(i)
        gather_rows(row_buf, v_parts, gv_row, hv_x)
        if first:
            norm_now = small_end(0)
            sends_f.drain()
        lax.fori_loop(0, rows, ready(v_row, d_row, x_row), 0)
        sends_s.drain()
        here = direction[...]
        dots = fold((errors[...] if first else diag[...]) * here * here)
        if first:
            sweep(x_row, 1, 1, row_part, 0, count)
            extra = pl.ds(rhs, EXTRA)

            def weigh(b, carry):
                held = held_row[b]
                return carry + fold(column_image(b, extra)[:1] * (held * held))

            dots = lax.fori_loop(0, rows, weigh, dots)

            def weigh_col(a, carry):
                held = held_col[a]
                return carry + fold(row_image(a, extra)[:1] * (held * held))

            dots = lax.fori_loop(0, cols, weigh_col, dots)

        def meet(b, carry):
            return carry + 2.0 * fold(column_image(b, pl.ds(0, rhs)) * held_row[b])

        dots = lax.fori_loop(0, rows, meet, dots)
        small_start(sends_s, 1, lane_sums(dots))
        if not first:
            sweep(x_row, 1, 1, row_part, 0, half)
            small_middle(sends_s, 1)
            sweep(x_row, 1, 1, row_part, half, count)
        for k in range(cols):
            a = to_col[k][1] if k < cols - 1 else c
            for n, (start, size) in enumerate(parts):
                span = pl.ds(start, size)
                c_stage[k, span] = row_image(a, span)
                if k < cols - 1:
                    sends_r.go(remote(c_stage.at[k, span], c_got.at[k, span],
                                      qc.at[k, n], rc.at[k, n], to_col[k]))
        if first:
            small_middle(sends_s, 1)

        for i in range(outer - 1):
            q = order[i]
            below = q < z
            way = jnp.where(below, 0, 1)
            more = jnp.where(below, z + 1 < outer, z > 0)
            target = (jnp.where(below, r - inner, r + inner), c)
            for n, (start, size) in enumerate(parts):
                span = pl.ds(start, size)
                z_stage[i, span] = joined(i, n, span)
                copy = remote(z_stage.at[i, span], z_got.at[way, q, span],
                              qz.at[i, n], rz.at[way, q, n], target)

                @pl.when(more)
                def _():
                    copy.wait_recv()
                    z_stage[i, span] += z_got[way, q, span]

                sends_r.go(copy)
        for n, (start, size) in enumerate(parts):
            span = pl.ds(start, size)
            for k, q in enumerate(from_col):
                block = c_got.at[k, span]
                remote(block, block, qc.at[k, n], rc.at[k, n], to_col[k]).wait_recv()
            value = c_stage[cols - 1, span]
            for k in range(cols - 1):
                value = value + c_got[k, span]
            product[span] = value + joined(outer - 1, n, span)
            for way, there in enumerate((has_high, has_low)):
                @pl.when(there)
                def _():
                    block = z_got.at[way, z, span]
                    remote(block, block, qz.at[0, n], rz.at[way, z, n],
                           high if way == 0 else low).wait_recv()
                    product[span] += z_got[way, z, span]
        alpha = norm_now / small_end(1)
        step = column(alpha, rhs, tile)
        if first:
            diag[...] = errors[...] + product[rhs:rhs + 1]
        image = diag[...] * here + product[:rhs]
        inc_out[...] += step * here
        residual = res_out[...] - step * image
        res_out[...] = residual
        sends_v.drain()
        if repeat + 1 < ITERS:
            v_row[repeat + 1, r] = residual
            v_col[repeat + 1, c] = residual
            row_buf, col_buf = v_row.at[repeat + 1], v_col.at[repeat + 1]
            sends_s.drain()
            small_start(sends_s, 0, lane_sums(fold(residual * residual)))
            gather_start(sends_v, row_buf.at[r], row_buf, col_buf, v_parts,
                         gv_row, gv_col, hv_z, hv_x, hv_c)
            relay = gather_relay(sends_v, row_buf, v_parts, gv_row, hv_z, hv_x)
    sends_r.drain()
    sends_s.drain()
    sends_v.drain()


def shards(rows, cols, innovations, obs_factors, component, obs_error, coupling, tile_slots):
    slots = tile_slots[0, 0]
    rhs, tile = innovations.shape
    depth = obs_factors.shape[0]
    count = slots.shape[0]
    outer, inner = legs(rows)
    sides = max(inner - 1, 1)
    tall, wide = depth + EXTRA, rhs + EXTRA
    nf = len(pieces(tall, PIECE_FACTORS))
    nv = len(pieces(rhs, PIECE))
    nr = max(len(pieces(wide, PIECE_FIRST)), nv)
    dma = pltpu.SemaphoreType.DMA
    scratch = [
        pltpu.VMEM((rows, tall, tile), F32),
        pltpu.VMEM((cols, tall, tile), F32),
        pltpu.VMEM((ITERS, rows, rhs, tile), F32),
        pltpu.VMEM((ITERS, cols, rhs, tile), F32),
        pltpu.VMEM((rows, rhs, tile), F32),
        pltpu.VMEM((cols, rhs, tile), F32),
        pltpu.VMEM((rows, 2 * rhs + ONES, tile), BF16),
        pltpu.VMEM((cols, 2 * rhs + ONES, tile), BF16),
        pltpu.VMEM((cols, tile, tile), BF16),
        pltpu.VMEM((count, tile, tile), BF16),
        pltpu.VMEM((count, tile, tile), BF16),
        pltpu.VMEM((count + 1, wide, tile), F32),
        pltpu.VMEM((count + 1, wide, tile), F32),
        pltpu.SMEM((rows * cols,), jnp.int32),
        pltpu.VMEM((2, cols, 8, 128), F32),
        pltpu.VMEM((2, rows, 8, 128), F32),
        pltpu.VMEM((outer, sides, wide, tile), F32),
        pltpu.VMEM((ITERS, outer, sides, wide, tile), F32),
        pltpu.VMEM((outer, wide, tile), F32),
        pltpu.VMEM((2, outer, wide, tile), F32),
        pltpu.VMEM((cols, wide, tile), F32),
        pltpu.VMEM((cols, wide, tile), F32),
        pltpu.VMEM((wide, tile), F32),
        pltpu.VMEM((1, tile), F32),
        pltpu.VMEM((rhs, tile), F32),
        dma((rows, nf)), dma((cols, nf)), dma((rows, nv)), dma((cols, nv)),
        dma((2, outer, nf)), dma((2, outer, sides, nf)), dma((cols, nf)),
        dma((2, outer, nv)), dma((2, outer, sides, nv)), dma((cols, nv)),
        dma((ITERS, outer, sides, nr)), dma((2, outer, nr)), dma((cols, nr)),
        dma((outer, sides, nr)), dma((outer, nr)), dma((cols, nr)),
        dma((2, cols)), dma((2, rows)), dma((2, cols)), dma((2, rows)),
    ]
    out = jax.ShapeDtypeStruct((rhs, tile), F32)
    return pl.pallas_call(
        functools.partial(kernel, rows, cols),
        out_shape=(out, out),
        in_specs=[VMEM] * 4 + [SMEM] * 2,
        out_specs=(VMEM, VMEM),
        scratch_shapes=scratch,
        compiler_params=pltpu.CompilerParams(collective_id=0, has_side_effects=True),
    )(innovations, obs_factors, component.reshape(1, tile), obs_error.reshape(1, tile),
      coupling, slots)


def solution(mesh):
    return jax.shard_map(
        functools.partial(shards, mesh.shape["row"], mesh.shape["col"]),
        mesh=mesh,
        in_specs=(
            P(None, ("row", "col")),
            P(None, ("row", "col")),
            P(("row", "col")),
            P(("row", "col")),
            P(),
            P("row", "col", None, None),
        ),
        out_specs=(P(None, ("row", "col")), P(None, ("row", "col"))),
        check_vma=False,
    )
```

```python
import functools
import math

import jax
import jax.numpy as jnp
from jax import lax
from jax.experimental import pallas as pl
from jax.experimental.pallas import tpu as pltpu
from jax.sharding import PartitionSpec as P

ITERS = 3
length_sq = 12.0
MESH = pl.DeviceIdType.MESH
VMEM = pl.BlockSpec(memory_space=pltpu.VMEM)
SMEM = pl.BlockSpec(memory_space=pltpu.SMEM)
F32, BF16 = jnp.float32, jnp.bfloat16
PIECE_FACTORS = 24
PIECE_FIRST = 40
PIECE = 32
EXTRA = 8
ONES = 16
DEAD = 1000.0


def legs(rows):
    outer = 4 if rows % 4 == 0 else rows
    return outer, rows // outer


def pieces(height, size):
    return [(start, min(size, height - start)) for start in range(0, height, size)]


def remote(src, dst, send, recv, device):
    return pltpu.make_async_remote_copy(
        src_ref=src, dst_ref=dst, send_sem=send, recv_sem=recv,
        device_id=device, device_id_type=MESH,
    )


def split2(x):
    top = x.astype(BF16)
    return top, (x - top.astype(F32)).astype(BF16)


def split3(x):
    first = x.astype(BF16)
    rest = x - first.astype(F32)
    second = rest.astype(BF16)
    return first, second, (rest - second.astype(F32)).astype(BF16)


def fold(x):
    total = x[:, :128]
    for start in range(128, x.shape[1], 128):
        total = total + x[:, start:start + 128]
    return total


def lane_sums(x):
    rest = 128 - x.shape[0]
    square = jnp.concatenate([x, jnp.zeros((rest, 128), F32)], axis=0) if rest else x
    return jnp.sum(jnp.transpose(square), axis=0, keepdims=True)


def column(row, height, width):
    square = jnp.transpose(jnp.broadcast_to(row, (128, 128)))[:height]
    return jnp.concatenate([square] * (width // 128), axis=1)


def stack_rows(values, width):
    place = lax.broadcasted_iota(jnp.int32, (16, width), 0)
    total = jnp.zeros((16, width), F32)
    for n, value in enumerate(values):
        total = jnp.where(place == n, value.astype(F32), total)
    return total.astype(BF16)


class Sends:
    def __init__(self):
        self.held = []

    def go(self, copy, when=None):
        if when is None:
            copy.start()
        else:
            pl.when(when)(copy.start)
        self.held.append((copy, when))

    def drain(self):
        for copy, when in self.held:
            if when is None:
                copy.wait_send()
            else:
                pl.when(when)(copy.wait_send)
        self.held = []


def kernel(rows, cols, innov, factors, labels, errors, coupling, slots, inc_out, res_out,
           f_row, f_col, v_row, v_col, d_row, d_col, x_row, x_col, left, t_high, t_low,
           col_part, row_part, where_slot, s1, s2,
           x_stage, x_got, z_stage, z_got, c_stage, c_got, product, diag, direction,
           gf_row, gf_col, gv_row, gv_col, hf_z, hf_x, hf_c, hv_z, hv_x, hv_c,
           rx, rz, rc, qx, qz, qc, r1, r2, q1, q2):
    r, c = lax.axis_index("row"), lax.axis_index("col")
    outer, inner = legs(rows)
    z, w = lax.div(r, inner), lax.rem(r, inner)
    has_low, has_high = z > 0, z < outer - 1
    low, high = (r - inner, c), (r + inner, c)
    to_col = [(r, lax.rem(c + k, cols)) for k in range(1, cols)]
    to_row = [(lax.rem(r + k, rows), c) for k in range(1, rows)]
    from_col = [lax.rem(c + cols - k, cols) for k in range(1, cols)]
    from_row = [lax.rem(r + rows - k, rows) for k in range(1, rows)]
    side_of = [lax.rem(w + j, inner) for j in range(1, inner)]
    back_of = [lax.rem(w + inner - j, inner) for j in range(1, inner)]
    rhs, tile = innov.shape
    depth = factors.shape[0]
    count = slots.shape[0]

    def gather_start(sends, source, row_buf, col_buf, parts, g_row, g_col, h_z, h_x, h_c):
        for n, (start, size) in enumerate(parts):
            span = pl.ds(start, size)
            mine = source.at[span]
            target = row_buf.at[r, span]
            sends.go(remote(mine, target, h_z.at[0, 0, n], g_row.at[r, n], low), has_low)
            sends.go(remote(mine, target, h_z.at[1, 0, n], g_row.at[r, n], high), has_high)
            for j, side in enumerate(side_of):
                sends.go(remote(mine, target, h_x.at[0, 0, j, n], g_row.at[r, n],
                                (z * inner + side, c)))
            for k, device in enumerate(to_col):
                sends.go(remote(mine, col_buf.at[c, span], h_c.at[k, n], g_col.at[c, n], device))

    def gather_relay(sends, row_buf, parts, g_row, h_z, h_x):
        for step in range(1, outer):
            for n, (start, size) in enumerate(parts):
                span = pl.ds(start, size)
                for way in range(2):
                    slot = r - step * inner if way else r + step * inner
                    there = z - step >= 0 if way else z + step < outer
                    onward = has_high if way else has_low
                    block = row_buf.at[slot, span]
                    arrival = remote(block, block, h_z.at[way, step, n], g_row.at[slot, n],
                                     high if way else low)
                    pl.when(there)(arrival.wait_recv)
                    sends.go(arrival, there & onward)
                    for j, side in enumerate(side_of):
                        sends.go(remote(block, block, h_x.at[way, step, j, n], g_row.at[slot, n],
                                        (z * inner + side, c)), there)
            yield step

    def gather_cols(col_buf, parts, g_col, h_c):
        for n, (start, size) in enumerate(parts):
            for k, q in enumerate(from_col):
                block = col_buf.at[q, pl.ds(start, size)]
                remote(block, block, h_c.at[k, n], g_col.at[q, n], to_col[k]).wait_recv()

    def gather_rows(row_buf, parts, g_row, h_x):
        for n, (start, size) in enumerate(parts):
            for plane in range(outer):
                for j, back in enumerate(back_of):
                    slot = plane * inner + back
                    block = row_buf.at[slot, pl.ds(start, size)]
                    remote(block, block, h_x.at[0, 0, j, n], g_row.at[slot, n],
                           (z * inner + back, c)).wait_recv()

    def small_start(sends, kind, value):
        s1[kind, c] = jnp.broadcast_to(value, (8, 128))
        mine = s1.at[kind, c, pl.ds(0, 1)]
        for k, device in enumerate(to_col):
            sends.go(remote(mine, mine, q1.at[kind, k], r1.at[kind, k], device))

    def small_middle(sends, kind):
        for k, q in enumerate(from_col):
            there = s1.at[kind, q, pl.ds(0, 1)]
            remote(there, there, q1.at[kind, k], r1.at[kind, k], to_col[k]).wait_recv()
        total = s1[kind, 0, :1]
        for k in range(1, cols):
            total = total + s1[kind, k, :1]
        s2[kind, r] = jnp.broadcast_to(total, (8, 128))
        mine = s2.at[kind, r, pl.ds(0, 1)]
        for k, device in enumerate(to_row):
            sends.go(remote(mine, mine, q2.at[kind, k], r2.at[kind, k], device))

    def small_end(kind):
        for k, q in enumerate(from_row):
            there = s2.at[kind, q, pl.ds(0, 1)]
            remote(there, there, q2.at[kind, k], r2.at[kind, k], to_row[k]).wait_recv()
        total = s2[kind, 0, :1]
        for k in range(1, rows):
            total = total + s2[kind, k, :1]
        return total

    barrier = pltpu.get_barrier_semaphore()
    for device in to_col + to_row:
        pl.semaphore_signal(barrier, inc=1, device_id=device, device_id_type=MESH)

    scale = math.sqrt(2.0 / (length_sq * math.log(2.0)))
    own = jnp.concatenate(
        [factors[...] * scale, jnp.broadcast_to(labels[...].astype(F32), (EXTRA, tile))], axis=0
    )
    f_row[r] = own
    f_col[c] = own
    start_values = innov[...]
    rr_part = lane_sums(fold(start_values * start_values))
    pl.semaphore_wait(barrier, len(to_col) + len(to_row))

    f_parts = pieces(depth + EXTRA, PIECE_FACTORS)
    v_parts = pieces(rhs, PIECE)
    sends_f, sends_v, sends_s, sends_r = Sends(), Sends(), Sends(), Sends()
    small_start(sends_s, 0, rr_part)
    gather_start(sends_f, f_row.at[r], f_row, f_col, f_parts, gf_row, gf_col, hf_z, hf_x, hf_c)
    gather_start(sends_v, innov, v_row.at[0], v_col.at[0], v_parts,
                 gv_row, gv_col, hv_z, hv_x, hv_c)

    v_row[0, r] = start_values
    v_col[0, c] = start_values
    direction[...] = start_values
    inc_out[...] = jnp.zeros_like(start_values)
    res_out[...] = start_values
    for part in (col_part, row_part):
        part[count] = jnp.zeros(part.shape[1:], F32)

    def locate(n, carry):
        a, b = lax.div(n, rows), lax.rem(n, rows)
        found = jnp.int32(count)
        for s in range(count):
            hit = (slots[s, 2] > 0) & (slots[s, 0] == a) & (slots[s, 1] == b)
            found = jnp.where(hit, s, found)
        where_slot[n] = found
        return carry

    lax.fori_loop(0, rows * cols, locate, 0)

    logs = [[jnp.log(jnp.full((1, tile), coupling[i, j], F32)) * (1.0 / math.log(2.0))
             for j in range(2)] for i in range(2)]
    one = jnp.ones((1, tile), F32)
    nothing = jnp.zeros((tile - 6 * depth - 16, tile), BF16)

    relay_f = gather_relay(sends_f, f_row, f_parts, gf_row, hf_z, hf_x)
    next(relay_f)
    small_middle(sends_s, 0)
    gather_cols(f_col, f_parts, gf_col, hf_c)

    def prepare(a, carry):
        g = f_col[a, :depth]
        label = f_col[a, depth:depth + 1]
        g1, g2, g3 = split3(g)
        m = split3(-0.5 * jnp.sum(g * g, axis=0, keepdims=True))
        extra = stack_rows(list(m) + [one] * 3 + [label] * 3, tile)
        stack = jnp.concatenate([g1, g1, g2, g2, g1, g3, extra, nothing], axis=0)
        left[a] = jnp.transpose(stack)
        return carry

    lax.fori_loop(0, cols, prepare, 0)
    for _ in relay_f:
        pass
    relay = gather_relay(sends_v, v_row.at[0], v_parts, gv_row, hv_z, hv_x)
    next(relay)
    gather_rows(f_row, f_parts, gf_row, hf_x)

    def build(s, carry):
        a, b = slots[s, 0], slots[s, 1]
        g = f_row[b, :depth]
        label = f_row[b, depth:depth + 1]
        g1, g2, g3 = split3(g)
        gone = jnp.where(slots[s, 2] > 0, 0.0, DEAD)
        base = -0.5 * jnp.sum(g * g, axis=0, keepdims=True)
        base = base + (logs[0][0] + label * (logs[0][1] - logs[0][0])) - gone
        slope = (logs[1][0] - logs[0][0]) + label * (
            (logs[1][1] - logs[1][0]) - (logs[0][1] - logs[0][0]))
        extra = stack_rows([one] * 3 + list(split3(base)) + list(split3(slope)), tile)
        stack = jnp.concatenate([g1, g2, g1, g2, g3, g1, extra, nothing], axis=0)
        value = jnp.exp2(jnp.dot(left[a], stack, preferred_element_type=F32))
        top, rest = split2(value)
        t_high[s] = top
        t_low[s] = rest
        return carry

    half = count // 2
    lax.fori_loop(0, half, build, 0, unroll=2)
    next(relay)
    lax.fori_loop(half, count, build, 0, unroll=2)

    ones_rows = jnp.ones((ONES, tile), BF16)
    bottom = rhs + ONES

    def put(target, index, value):
        top, rest = split2(value)
        target[index, :rhs] = top
        target[index, rhs:bottom] = ones_rows
        target[index, bottom:] = rest

    def sweep(values, which, side, part, begin, end):
        dims = (((1,), (side,)), ((), ()))

        def one_slot(s, carry):
            index = slots[s, which]
            wide = lax.dot_general(values[index], t_high[s], dims, preferred_element_type=F32)
            rest = lax.dot_general(values[index, :bottom], t_low[s], dims,
                                   preferred_element_type=F32)
            part[s, :rhs] = wide[:rhs] + (wide[bottom:] + rest[:rhs])
            part[s, rhs:] = wide[rhs:rhs + EXTRA] + rest[rhs:rhs + EXTRA]
            return carry

        lax.fori_loop(begin, end, one_slot, 0, unroll=2)

    def column_image(b, span):
        total = col_part[where_slot[b], span]
        for a in range(1, cols):
            total = total + col_part[where_slot[a * rows + b], span]
        return total

    def row_image(a, span):
        total = row_part[where_slot[a * rows], span]
        for b in range(1, rows):
            total = total + row_part[where_slot[a * rows + b], span]
        return total

    order = []
    lower_half = z < outer // 2
    for i in range(outer - 1):
        down = outer - 1 - i
        order.append(jnp.where(lower_half, jnp.where(down <= z, down - 1, down),
                               jnp.where(i >= z, i + 1, i)))
    order.append(z)

    for repeat in range(ITERS):
        first = repeat == 0
        row_buf, col_buf = v_row.at[repeat], v_col.at[repeat]
        parts = pieces(rhs + EXTRA, PIECE_FIRST) if first else pieces(rhs, PIECE)
        if not first:
            next(relay)
            small_middle(sends_s, 0)
            next(relay)
        gather_cols(col_buf, v_parts, gv_col, hv_c)
        weight = None
        if not first:
            norm_next = small_end(0)
            weight = column(norm_next / norm_now, rhs, tile)
            norm_now = norm_next
            direction[...] = res_out[...] + weight * direction[...]

        def ready(fresh, kept, target):
            def one_block(b, carry):
                value = fresh[repeat, b]
                if repeat:
                    value = value + weight * (fresh[0, b] if repeat == 1 else kept[b])
                    kept[b] = value
                put(target, b, value)
                return carry

            return one_block

        lax.fori_loop(0, cols, ready(v_col, d_col, x_col), 0)
        sweep(x_col, 0, 0, col_part, 0, half)
        for _ in relay:
            pass
        sweep(x_col, 0, 0, col_part, half, count)
        held_col = v_col.at[0] if first else d_col
        held_row = v_row.at[0] if first else d_row
        sends_r.drain()

        def send_across(i):
            for j, side in enumerate(side_of):
                for n, (start, size) in enumerate(parts):
                    span = pl.ds(start, size)
                    x_stage[i, j, span] = column_image(order[i] * inner + side, span)
                    sends_r.go(remote(x_stage.at[i, j, span], x_got.at[repeat, i, j, span],
                                      qx.at[i, j, n], rx.at[repeat, i, j, n], (z * inner + side, c)))

        def joined(i, n, span):
            value = column_image(order[i] * inner + w, span)
            for j in range(inner - 1):
                block = x_got.at[repeat, i, j, span]
                remote(block, block, qx.at[i, j, n], rx.at[repeat, i, j, n],
                       (z * inner + side_of[j], c)).wait_recv()
                value = value + x_got[repeat, i, j, span]
            return value

        def home_steps():
            for i in range(outer - 1):
                q = order[i]
                target = (q * inner + w, c)
                for n, (start, size) in enumerate(parts):
                    span = pl.ds(start, size)
                    z_stage[i, span] = joined(i, n, span)
                    sends_r.go(remote(z_stage.at[i, span], z_got.at[z, span],
                                      qz.at[i, n], rz.at[z, n], target))
                yield i

        homeward = home_steps()
        for i in range(outer):
            send_across(i)
        gather_rows(row_buf, v_parts, gv_row, hv_x)
        if first:
            norm_now = small_end(0)
            sends_f.drain()
        lax.fori_loop(0, rows, ready(v_row, d_row, x_row), 0)
        sends_s.drain()
        here = direction[...]
        dots = fold((errors[...] if first else diag[...]) * here * here)
        if first:
            sweep(x_row, 1, 1, row_part, 0, count)
            extra = pl.ds(rhs, EXTRA)

            def weigh(b, carry):
                held = held_row[b]
                return carry + fold(column_image(b, extra)[:1] * (held * held))

            dots = lax.fori_loop(0, rows, weigh, dots)

            def weigh_col(a, carry):
                held = held_col[a]
                return carry + fold(row_image(a, extra)[:1] * (held * held))

            dots = lax.fori_loop(0, cols, weigh_col, dots)

        def meet(b, carry):
            return carry + 2.0 * fold(column_image(b, pl.ds(0, rhs)) * held_row[b])

        dots = lax.fori_loop(0, rows, meet, dots)
        small_start(sends_s, 1, lane_sums(dots))
        if not first:
            sweep(x_row, 1, 1, row_part, 0, half)
            small_middle(sends_s, 1)
            next(homeward)
            sweep(x_row, 1, 1, row_part, half, count)
            next(homeward)
        for k in range(cols):
            a = to_col[k][1] if k < cols - 1 else c
            for n, (start, size) in enumerate(parts):
                span = pl.ds(start, size)
                c_stage[k, span] = row_image(a, span)
                if k < cols - 1:
                    sends_r.go(remote(c_stage.at[k, span], c_got.at[k, span],
                                      qc.at[k, n], rc.at[k, n], to_col[k]))
        if first:
            small_middle(sends_s, 1)

        for _ in homeward:
            pass
        for n, (start, size) in enumerate(parts):
            span = pl.ds(start, size)
            for k, q in enumerate(from_col):
                block = c_got.at[k, span]
                remote(block, block, qc.at[k, n], rc.at[k, n], to_col[k]).wait_recv()
            value = c_stage[cols - 1, span]
            for k in range(cols - 1):
                value = value + c_got[k, span]
            product[span] = value + joined(outer - 1, n, span)
            for i in range(outer - 1):
                block = z_got.at[order[outer - 2 - i], span]
                remote(block, block, qz.at[i, n], rz.at[order[outer - 2 - i], n], low).wait_recv()
                product[span] += z_got[order[outer - 2 - i], span]
        alpha = norm_now / small_end(1)
        step = column(alpha, rhs, tile)
        if first:
            diag[...] = errors[...] + product[rhs:rhs + 1]
        image = diag[...] * here + product[:rhs]
        inc_out[...] += step * here
        residual = res_out[...] - step * image
        res_out[...] = residual
        sends_v.drain()
        if repeat + 1 < ITERS:
            v_row[repeat + 1, r] = residual
            v_col[repeat + 1, c] = residual
            row_buf, col_buf = v_row.at[repeat + 1], v_col.at[repeat + 1]
            sends_s.drain()
            small_start(sends_s, 0, lane_sums(fold(residual * residual)))
            gather_start(sends_v, row_buf.at[r], row_buf, col_buf, v_parts,
                         gv_row, gv_col, hv_z, hv_x, hv_c)
            relay = gather_relay(sends_v, row_buf, v_parts, gv_row, hv_z, hv_x)
    sends_r.drain()
    sends_s.drain()
    sends_v.drain()


def shards(rows, cols, innovations, obs_factors, component, obs_error, coupling, tile_slots):
    slots = tile_slots[0, 0]
    rhs, tile = innovations.shape
    depth = obs_factors.shape[0]
    count = slots.shape[0]
    outer, inner = legs(rows)
    sides = max(inner - 1, 1)
    tall, wide = depth + EXTRA, rhs + EXTRA
    nf = len(pieces(tall, PIECE_FACTORS))
    nv = len(pieces(rhs, PIECE))
    nr = max(len(pieces(wide, PIECE_FIRST)), nv)
    dma = pltpu.SemaphoreType.DMA
    scratch = [
        pltpu.VMEM((rows, tall, tile), F32),
        pltpu.VMEM((cols, tall, tile), F32),
        pltpu.VMEM((ITERS, rows, rhs, tile), F32),
        pltpu.VMEM((ITERS, cols, rhs, tile), F32),
        pltpu.VMEM((rows, rhs, tile), F32),
        pltpu.VMEM((cols, rhs, tile), F32),
        pltpu.VMEM((rows, 2 * rhs + ONES, tile), BF16),
        pltpu.VMEM((cols, 2 * rhs + ONES, tile), BF16),
        pltpu.VMEM((cols, tile, tile), BF16),
        pltpu.VMEM((count, tile, tile), BF16),
        pltpu.VMEM((count, tile, tile), BF16),
        pltpu.VMEM((count + 1, wide, tile), F32),
        pltpu.VMEM((count + 1, wide, tile), F32),
        pltpu.SMEM((rows * cols,), jnp.int32),
        pltpu.VMEM((2, cols, 8, 128), F32),
        pltpu.VMEM((2, rows, 8, 128), F32),
        pltpu.VMEM((outer, sides, wide, tile), F32),
        pltpu.VMEM((ITERS, outer, sides, wide, tile), F32),
        pltpu.VMEM((outer, wide, tile), F32),
        pltpu.VMEM((outer, wide, tile), F32),
        pltpu.VMEM((cols, wide, tile), F32),
        pltpu.VMEM((cols, wide, tile), F32),
        pltpu.VMEM((wide, tile), F32),
        pltpu.VMEM((1, tile), F32),
        pltpu.VMEM((rhs, tile), F32),
        dma((rows, nf)), dma((cols, nf)), dma((rows, nv)), dma((cols, nv)),
        dma((2, outer, nf)), dma((2, outer, sides, nf)), dma((cols, nf)),
        dma((2, outer, nv)), dma((2, outer, sides, nv)), dma((cols, nv)),
        dma((ITERS, outer, sides, nr)), dma((outer, nr)), dma((cols, nr)),
        dma((outer, sides, nr)), dma((outer, nr)), dma((cols, nr)),
        dma((2, cols)), dma((2, rows)), dma((2, cols)), dma((2, rows)),
    ]
    out = jax.ShapeDtypeStruct((rhs, tile), F32)
    return pl.pallas_call(
        functools.partial(kernel, rows, cols),
        out_shape=(out, out),
        in_specs=[VMEM] * 4 + [SMEM] * 2,
        out_specs=(VMEM, VMEM),
        scratch_shapes=scratch,
        compiler_params=pltpu.CompilerParams(collective_id=0, has_side_effects=True),
    )(innovations, obs_factors, component.reshape(1, tile), obs_error.reshape(1, tile),
      coupling, slots)


def solution(mesh):
    return jax.shard_map(
        functools.partial(shards, mesh.shape["row"], mesh.shape["col"]),
        mesh=mesh,
        in_specs=(
            P(None, ("row", "col")),
            P(None, ("row", "col")),
            P(("row", "col")),
            P(("row", "col")),
            P(),
            P("row", "col", None, None),
        ),
        out_specs=(P(None, ("row", "col")), P(None, ("row", "col"))),
        check_vma=False,
    )
```
